32 devices in a mesh: grp: 4 (over y, core), loc: 8 (over z, x).
Axes of the slice: x: 2, y: 2, z: 4, core: 2. Of those that a mesh axis runs over, the one named last changes fastest.
Arguments:
- tokens: bfloat16 [8192, 1024], P(('grp', 'loc')), may hold values from -6 to 6
- w_gate: bfloat16 [32, 1024, 2816], P(('grp', 'loc')), may hold values from -0.1875 to 0.1875
- w_up: bfloat16 [32, 1024, 2816], P(('grp', 'loc')), may hold values from -0.1875 to 0.1875
- w_down: bfloat16 [32, 2816, 1024], P(('grp', 'loc')), may hold values from -0.109375 to 0.109375
- chosen: int32 [32, 128], replicated, may hold values from -1 to 8191, as said below
- gate_weights: float32 [32, 128], replicated, may hold values from 0.05 to 1
Outputs:
- combined: bfloat16 [8192, 1024], P(('grp', 'loc'))
The draws below stay inside these ranges and needn't reach their ends.
Inputs may be any that keep to these rules, and one draw needn't show every extreme that they name: `chosen`: each entry is a token index or -1 for an empty slot, empty slots anywhere in a row. One expert's row names a token at most once. At most 8 entries of one expert's row lie among the 256 tokens of one device, and every expert has exactly 8 from some device. Some expert has no empty slot.
All inputs are finite; a program needn't handle non-finite values.
Results may differ from the reference program's by a relative error of at most 0.0085.
Values may be sent and summed in bfloat16 or wider, within the bound.
No kernel may reach another device: no remote copies, remote signals or barrier semaphores. Data moves between devices by JAX's collectives and lax.ppermute only.
A program may use at most 128 MiB of HBM per device.

```python
import math
import jax
import jax.numpy as jnp
from jax import lax

D = 1024
FF = 2816
TOK_DEV = 256
PAIR_MOST = 8
EXPERTS = 32
CAP = 128
TOKENS = 8192


def draw_chosen(key, part):
    key_level, key_count, key_order, key_full, key_local, key_shuffle = jax.random.split(key, 6)
    load_level = jax.random.randint(key_level, (EXPERTS,), 0, 4)
    ceiling = jnp.minimum(jnp.array([5, 7, 9, 9], jnp.int32)[load_level], PAIR_MOST + 1)
    counts = jax.random.randint(key_count, (EXPERTS, EXPERTS), 0, ceiling[None, :])
    order_scores = jax.random.randint(key_order, (EXPERTS, EXPERTS), 0, 1 << 18) * EXPERTS + jnp.arange(EXPERTS)[None, :]
    source_order = jnp.argsort(order_scores, axis=1).astype(jnp.int32)
    ordered = jnp.take_along_axis(counts, source_order, axis=1)
    full_expert = jax.random.randint(key_full, (), 0, EXPERTS)
    row_iota = jnp.arange(EXPERTS)[:, None]
    column_iota = jnp.arange(EXPERTS)[None, :]
    ordered = jnp.where((column_iota == 0) | (row_iota == full_expert), PAIR_MOST, ordered)
    before = jnp.cumsum(ordered, axis=1) - ordered
    kept_count = jnp.minimum(jnp.maximum(CAP - before, 0), ordered)
    scores = jax.random.randint(key_local, (EXPERTS, EXPERTS, TOK_DEV), 0, 1 << 18) * TOK_DEV + jnp.arange(TOK_DEV)[None, None, :]
    local_pick = jnp.argsort(scores, axis=2)[:, :, :PAIR_MOST].astype(jnp.int32)
    global_id = source_order[:, :, None] * TOK_DEV + local_pick
    pair_iota = jnp.arange(PAIR_MOST)[None, None, :]
    is_valid = pair_iota < kept_count[:, :, None]
    slot_index = jnp.where(is_valid, before[:, :, None] + pair_iota, CAP)
    expert_ids = jnp.broadcast_to(row_iota[:, :, None], slot_index.shape)
    slot_table = jnp.full((EXPERTS, CAP), -1, jnp.int32).at[expert_ids, slot_index].set(global_id.astype(jnp.int32), mode='drop')
    shuffle_scores = jax.random.randint(key_shuffle, (EXPERTS, CAP), 0, 1 << 18) * CAP + jnp.arange(CAP)[None, :]
    shuffle = jnp.argsort(shuffle_scores, axis=1)
    return jnp.take_along_axis(slot_table, shuffle, axis=1)


def block_scale(key, dims, pieces, least, top_value):
    def one(axis_at, blocks):
        steps = jax.random.uniform(jax.random.fold_in(jax.random.fold_in(key, 6), axis_at), (blocks,), jnp.float32, least / len(pieces), top_value / len(pieces))
        return jnp.repeat(jnp.exp(steps), dims[axis_at] // blocks).reshape((-1,) + (1,) * (len(dims) - axis_at - 1))

    loudness = one(*pieces[0])
    for cut in pieces[1:]:
        loudness = loudness * one(*cut)
    return loudness


def centred(stream_key, dims, scale, most, cuts=(), kind=jnp.bfloat16):
    gain = block_scale(stream_key, dims, cuts, -0.22, 0.18) if cuts else 1.0
    drawn = jax.random.normal(stream_key, dims, jnp.float32) * scale * gain
    return jnp.minimum(jnp.maximum(drawn, -most), most).astype(kind)


def setup_inputs(seed: int = 0) -> dict:
    splits = jax.random.split(jax.random.key(seed), 7)
    return {
        "tokens": centred(splits[0], (TOKENS, D), 1.0, 6.0, ((0, 32),)),
        "w_gate": centred(splits[1], (EXPERTS, D, FF), D ** -0.5, 0.1875, ((0, 32),)),
        "w_up": centred(splits[2], (EXPERTS, D, FF), D ** -0.5, 0.1875, ((0, 32),)),
        "w_down": centred(splits[3], (EXPERTS, FF, D), FF ** -0.5, 0.109375, ((0, 32),)),
        "chosen": draw_chosen(jax.random.fold_in(splits[6], 71), 0),
        "gate_weights": jnp.clip(jnp.exp(jax.random.uniform(splits[5], (EXPERTS, CAP), jnp.float32, math.log(0.05), math.log(1.0))), 0.05, 1.0),
    }


def reference(tokens, w_gate, w_up, w_down, chosen, gate_weights):
    token_total = tokens.shape[0]
    model_width = tokens.shape[1]
    padded = jnp.concatenate([tokens, jnp.zeros((1, model_width), tokens.dtype)], axis=0)

    def one_expert(expert, running):
        picks = lax.dynamic_index_in_dim(chosen, expert, 0, keepdims=False)
        is_live = picks >= 0
        row_index = jnp.where(is_live, picks, token_total).astype(jnp.int32)
        row_block = jnp.take(padded, row_index, axis=0)
        gate_mat = lax.dynamic_index_in_dim(w_gate, expert, 0, keepdims=False)
        up_mat = lax.dynamic_index_in_dim(w_up, expert, 0, keepdims=False)
        down_mat = lax.dynamic_index_in_dim(w_down, expert, 0, keepdims=False)
        gate_pre = jnp.dot(row_block, gate_mat, preferred_element_type=jnp.float32)
        up_pre = jnp.dot(row_block, up_mat, preferred_element_type=jnp.float32)
        hidden = (jax.nn.silu(gate_pre) * up_pre).astype(jnp.bfloat16)
        expert_out = jnp.dot(hidden, down_mat, preferred_element_type=jnp.float32).astype(jnp.bfloat16)
        slot_weight = jnp.where(is_live, lax.dynamic_index_in_dim(gate_weights, expert, 0, keepdims=False), 0.0)
        weighted = slot_weight[:, None] * expert_out.astype(jnp.float32)
        return running.at[row_index].add(weighted)

    running = jnp.zeros((token_total + 1, model_width), jnp.float32)
    running = lax.fori_loop(0, EXPERTS, one_expert, running)
    return running[:token_total].astype(jnp.bfloat16)
```

```python
import jax
import jax.numpy as jnp
from jax import lax
from jax.experimental import pallas as pl
from jax.experimental.pallas import tpu as pltpu
from jax.sharding import PartitionSpec as P

PAIR_MOST = 8
AXES = ("grp", "loc")
VMEM_SPEC = pl.BlockSpec(memory_space=pltpu.VMEM)
SMEM_SPEC = pl.BlockSpec(memory_space=pltpu.SMEM)
HBM_SPEC = pl.BlockSpec(memory_space=pltpu.HBM)


def dot(left, right):
    return jnp.dot(left, right, preferred_element_type=jnp.float32)


def ranks_of(mine):
    slots = mine.shape[1]
    row = lax.broadcasted_iota(jnp.int32, (slots, slots), 0)
    col = lax.broadcasted_iota(jnp.int32, (slots, slots), 1)
    earlier = (row < col).astype(jnp.bfloat16)
    return dot(mine.astype(jnp.bfloat16), earlier).astype(jnp.int32)


def pick_rows(device, chosen, token_count, values):
    experts, slots = chosen.shape
    local = chosen - device * token_count
    mine = (local >= 0) & (local < token_count)
    rank = jnp.where(mine, ranks_of(mine.astype(jnp.float32)), -1)
    shape = (experts, PAIR_MOST, slots)
    pair_slot = lax.broadcasted_iota(jnp.int32, shape, 1)
    hit = jnp.broadcast_to(rank[:, None, :], shape) == pair_slot
    rows = experts * PAIR_MOST

    def total(array, empty):
        spread = jnp.broadcast_to(array[:, None, :], shape)
        return jnp.sum(jnp.where(hit, spread, empty), axis=2, keepdims=True).reshape(rows, 1)

    index = total((local + 1).astype(jnp.float32), 0.0).astype(jnp.int32) - 1
    if values is None:
        return index
    return index, total(values, 0.0)


def dispatch_body(device_ref, chosen_hbm, tokens_hbm, out_ref, chosen_ref, tokens_ref, sems):
    copies = [
        pltpu.make_async_copy(chosen_hbm, chosen_ref, sems.at[0]),
        pltpu.make_async_copy(tokens_hbm, tokens_ref, sems.at[1]),
    ]
    for copy in copies:
        copy.start()
    copies[0].wait()
    token_count = tokens_ref.shape[0]
    index = pick_rows(device_ref[0], chosen_ref[...], token_count, None)
    token_iota = lax.broadcasted_iota(jnp.int32, (index.shape[0], token_count), 1)
    select = (index == token_iota).astype(jnp.bfloat16)
    copies[1].wait()
    out_ref[...] = dot(select, tokens_ref[...]).astype(jnp.bfloat16)


def table_body(device_ref, chosen_ref, weights_ref, high_ref, low_ref):
    token_count = high_ref.shape[1]
    index, weight = pick_rows(device_ref[0], chosen_ref[...], token_count, weights_ref[...])
    token_iota = lax.broadcasted_iota(jnp.int32, (index.shape[0], token_count), 1)
    table = jnp.where(index == token_iota, weight, 0.0)
    high = table.astype(jnp.bfloat16)
    high_ref[...] = high
    low_ref[...] = (table - high.astype(jnp.float32)).astype(jnp.bfloat16)


def expert_body(token_count, step, device_ref, chosen_ref, arrived_ref, gate_hbm, up_hbm, down_hbm,
                out_ref, gate_ref, up_ref, down_ref, sems):
    hidden_units = gate_ref.shape[1]
    chunks = []
    for number, start in enumerate(range(0, hidden_units, step)):
        span = pl.ds(start, min(step, hidden_units - start))
        copies = (
            pltpu.make_async_copy(gate_hbm.at[0, :, span], gate_ref.at[:, span], sems.at[0, number]),
            pltpu.make_async_copy(up_hbm.at[0, :, span], up_ref.at[:, span], sems.at[1, number]),
            pltpu.make_async_copy(down_hbm.at[0, span], down_ref.at[span], sems.at[2, number]),
        )
        for copy in copies:
            copy.start()
        chunks.append((span, copies))
    rows = arrived_ref.shape[0]
    devices = rows // PAIR_MOST
    slots = chosen_ref.shape[1]
    row = chosen_ref[pl.ds(device_ref[0], 1), :]
    first = lax.broadcasted_iota(jnp.int32, (devices, slots), 0) * token_count
    spread = jnp.broadcast_to(row, (devices, slots))
    mine = (spread >= first) & (spread < first + token_count)
    rank = jnp.where(mine, ranks_of(mine.astype(jnp.float32)), -1)
    shape = (devices, PAIR_MOST, slots)
    pair_slot = lax.broadcasted_iota(jnp.int32, shape, 1)
    hit = jnp.broadcast_to(rank[:, None, :], shape) == pair_slot
    place = jnp.where(hit, 1.0, 0.0).reshape(rows, slots).astype(jnp.bfloat16)
    block = lax.dot_general(
        place, arrived_ref[...], (((0,), (0,)), ((), ())), preferred_element_type=jnp.float32
    ).astype(jnp.bfloat16)
    total = jnp.zeros((slots, out_ref.shape[1]), jnp.float32)
    for span, (gate_copy, up_copy, down_copy) in chunks:
        gate_copy.wait()
        gate_pre = dot(block, gate_ref[:, span])
        up_copy.wait()
        up_pre = dot(block, up_ref[:, span])
        hidden = (gate_pre / (1.0 + jnp.exp(-gate_pre)) * up_pre).astype(jnp.bfloat16)
        down_copy.wait()
        total = total + dot(hidden, down_ref[span, :])
    out_ref[...] = dot(place, total.astype(jnp.bfloat16)).astype(jnp.bfloat16)


def combine_body(high_ref, low_ref, back_ref, out_ref):
    dims = (((0,), (0,)), ((), ()))
    back = back_ref[...]
    total = lax.dot_general(high_ref[...], back, dims, preferred_element_type=jnp.float32)
    total = total + lax.dot_general(low_ref[...], back, dims, preferred_element_type=jnp.float32)
    out_ref[...] = total.astype(jnp.bfloat16)


def shards(tokens, w_gate, w_up, w_down, chosen, gate_weights):
    device = lax.axis_index("grp") * lax.axis_size("loc") + lax.axis_index("loc")
    device = device.astype(jnp.int32).reshape(1)
    token_count, width = tokens.shape
    experts, _ = chosen.shape
    hidden_units = w_gate.shape[2]
    rows = experts * PAIR_MOST
    bf16 = jnp.bfloat16

    def exchange(block):
        block = block.reshape(experts, PAIR_MOST, width)
        block = lax.all_to_all(block, AXES, split_axis=0, concat_axis=0, tiled=True)
        return block.reshape(rows, width)

    small = pltpu.CompilerParams(vmem_limit_bytes=8 << 20)
    step = 512
    chunk_count = -(-hidden_units // step)

    def hbm(array):
        return pltpu.with_memory_space_constraint(array, pltpu.HBM)

    outgoing = pl.pallas_call(
        dispatch_body,
        in_specs=[SMEM_SPEC, HBM_SPEC, HBM_SPEC],
        out_specs=VMEM_SPEC,
        out_shape=jax.ShapeDtypeStruct((rows, width), bf16),
        scratch_shapes=[
            pltpu.VMEM(chosen.shape, chosen.dtype),
            pltpu.VMEM(tokens.shape, tokens.dtype),
            pltpu.SemaphoreType.DMA((2,)),
        ],
        compiler_params=small,
        name="dispatch",
    )(device, hbm(chosen), hbm(tokens))
    arrived = exchange(outgoing)
    high, low = pl.pallas_call(
        table_body,
        in_specs=[SMEM_SPEC, VMEM_SPEC, VMEM_SPEC],
        out_specs=[VMEM_SPEC] * 2,
        out_shape=[jax.ShapeDtypeStruct((rows, token_count), bf16)] * 2,
        compiler_params=small,
        cost_estimate=pl.CostEstimate(
            flops=1_000_000_000, bytes_accessed=4 * rows * token_count, transcendentals=0
        ),
        name="table",
    )(device, chosen, gate_weights)
    produced = pl.pallas_call(
        lambda *refs: expert_body(token_count, step, *refs),
        in_specs=[SMEM_SPEC] + [VMEM_SPEC] * 2 + [HBM_SPEC] * 3,
        out_specs=VMEM_SPEC,
        out_shape=jax.ShapeDtypeStruct((rows, width), bf16),
        scratch_shapes=[
            pltpu.VMEM((width, hidden_units), bf16),
            pltpu.VMEM((width, hidden_units), bf16),
            pltpu.VMEM((hidden_units, width), bf16),
            pltpu.SemaphoreType.DMA((3, chunk_count)),
        ],
        compiler_params=pltpu.CompilerParams(vmem_limit_bytes=40 << 20),
        name="expert",
    )(device, chosen, arrived, hbm(w_gate), hbm(w_up), hbm(w_down))
    returned = exchange(produced)
    return pl.pallas_call(
        combine_body,
        in_specs=[VMEM_SPEC] * 3,
        out_specs=VMEM_SPEC,
        out_shape=jax.ShapeDtypeStruct((token_count, width), bf16),
        compiler_params=small,
        name="combine",
    )(high, low, returned)


def solution(mesh):
    return jax.shard_map(
        shards,
        mesh=mesh,
        in_specs=(
            P(AXES, None),
            P(AXES, None, None),
            P(AXES, None, None),
            P(AXES, None, None),
            P(),
            P(),
        ),
        out_specs=P(AXES, None),
        check_vma=False,
    )
```

```python
import jax
import jax.numpy as jnp
from jax import lax
from jax.experimental import pallas as pl
from jax.experimental.pallas import tpu as pltpu
from jax.sharding import PartitionSpec as P

PAIR_MOST = 8
AXES = ("grp", "loc")
VMEM_SPEC = pl.BlockSpec(memory_space=pltpu.VMEM)
SMEM_SPEC = pl.BlockSpec(memory_space=pltpu.SMEM)
HBM_SPEC = pl.BlockSpec(memory_space=pltpu.HBM)


def dot(left, right):
    return jnp.dot(left, right, preferred_element_type=jnp.float32)


def ranks_of(mine):
    slots = mine.shape[1]
    row = lax.broadcasted_iota(jnp.int32, (slots, slots), 0)
    col = lax.broadcasted_iota(jnp.int32, (slots, slots), 1)
    earlier = (row < col).astype(jnp.bfloat16)
    return dot(mine.astype(jnp.bfloat16), earlier).astype(jnp.int32)


def pick_rows(device, chosen, token_count, values):
    experts, slots = chosen.shape
    local = chosen - device * token_count
    mine = (local >= 0) & (local < token_count)
    rank = jnp.where(mine, ranks_of(mine.astype(jnp.float32)), -1)
    shape = (experts, PAIR_MOST, slots)
    pair_slot = lax.broadcasted_iota(jnp.int32, shape, 1)
    hit = jnp.broadcast_to(rank[:, None, :], shape) == pair_slot
    rows = experts * PAIR_MOST

    def total(array, empty):
        spread = jnp.broadcast_to(array[:, None, :], shape)
        return jnp.sum(jnp.where(hit, spread, empty), axis=2, keepdims=True).reshape(rows, 1)

    index = total((local + 1).astype(jnp.float32), 0.0).astype(jnp.int32) - 1
    if values is None:
        return index
    return index, total(values, 0.0)


def dispatch_body(device_ref, chosen_hbm, tokens_hbm, out_ref, chosen_ref, tokens_ref, sems):
    copies = [
        pltpu.make_async_copy(chosen_hbm, chosen_ref, sems.at[0]),
        pltpu.make_async_copy(tokens_hbm, tokens_ref, sems.at[1]),
    ]
    for copy in copies:
        copy.start()
    copies[0].wait()
    token_count = tokens_ref.shape[0]
    index = pick_rows(device_ref[0], chosen_ref[...], token_count, None)
    token_iota = lax.broadcasted_iota(jnp.int32, (index.shape[0], token_count), 1)
    select = (index == token_iota).astype(jnp.bfloat16)
    copies[1].wait()
    out_ref[...] = dot(select, tokens_ref[...]).astype(jnp.bfloat16)


def expert_body(token_count, plan, device_ref, chosen_ref, arrived_ref, weights_hbm, gate_hbm, up_hbm, down_hbm,
                out_ref, high_ref, low_ref, weights_ref, gate_ref, up_ref, down_ref, sems, weights_sem):
    weights_copy = pltpu.make_async_copy(weights_hbm, weights_ref, weights_sem)
    chunks = []
    start = 0
    for number, size in enumerate(plan):
        span = pl.ds(start, size)
        start += size
        chunks.append((
            span,
            pltpu.make_async_copy(gate_hbm.at[0, :, span], gate_ref.at[:, span], sems.at[0, number]),
            pltpu.make_async_copy(up_hbm.at[0, :, span], up_ref.at[:, span], sems.at[1, number]),
            pltpu.make_async_copy(down_hbm.at[0, span], down_ref.at[span], sems.at[2, number]),
        ))
    for number in range(len(plan) + 1):
        if number < len(plan):
            chunks[number][1].start()
            chunks[number][2].start()
        if number == 0:
            weights_copy.start()
        else:
            chunks[number - 1][3].start()
    rows = arrived_ref.shape[0]
    devices = rows // PAIR_MOST
    slots = chosen_ref.shape[1]
    row = chosen_ref[pl.ds(device_ref[0], 1), :]
    first = lax.broadcasted_iota(jnp.int32, (devices, slots), 0) * token_count
    spread = jnp.broadcast_to(row, (devices, slots))
    mine = (spread >= first) & (spread < first + token_count)
    rank = jnp.where(mine, ranks_of(mine.astype(jnp.float32)), -1)
    shape = (devices, PAIR_MOST, slots)
    pair_slot = lax.broadcasted_iota(jnp.int32, shape, 1)
    hit = jnp.broadcast_to(rank[:, None, :], shape) == pair_slot
    place = jnp.where(hit, 1.0, 0.0).reshape(rows, slots).astype(jnp.bfloat16)
    block = lax.dot_general(
        place, arrived_ref[...], (((0,), (0,)), ((), ())), preferred_element_type=jnp.float32
    ).astype(jnp.bfloat16)
    total = jnp.zeros((slots, out_ref.shape[1]), jnp.float32)
    hidden = None
    for number in range(len(plan) + 1):
        before = hidden
        if number < len(plan):
            span, gate_copy, up_copy, _ = chunks[number]
            gate_copy.wait()
            gate_pre = dot(block, gate_ref[:, span])
            up_copy.wait()
            up_pre = dot(block, up_ref[:, span])
            hidden = (gate_pre / (1.0 + jnp.exp(-gate_pre)) * up_pre).astype(jnp.bfloat16)
        if number == 0:
            weights_copy.wait()
            table(device_ref[0], chosen_ref[...], weights_ref[...], high_ref, low_ref)
        else:
            span, _, _, down_copy = chunks[number - 1]
            down_copy.wait()
            total = total + dot(before, down_ref[span, :])
    out_ref[...] = dot(place, total.astype(jnp.bfloat16)).astype(jnp.bfloat16)


def table(device, chosen, weights, high_ref, low_ref):
    token_count = high_ref.shape[1]
    index, weight = pick_rows(device, chosen, token_count, weights)
    token_iota = lax.broadcasted_iota(jnp.int32, (index.shape[0], token_count), 1)
    full = jnp.where(index == token_iota, weight, 0.0)
    high = full.astype(jnp.bfloat16)
    high_ref[...] = high
    low_ref[...] = (full - high.astype(jnp.float32)).astype(jnp.bfloat16)


def combine_body(high_ref, low_ref, back_ref, out_ref):
    dims = (((0,), (0,)), ((), ()))
    back = back_ref[...]
    total = lax.dot_general(high_ref[...], back, dims, preferred_element_type=jnp.float32)
    total = total + lax.dot_general(low_ref[...], back, dims, preferred_element_type=jnp.float32)
    out_ref[...] = total.astype(jnp.bfloat16)


def shards(tokens, w_gate, w_up, w_down, chosen, gate_weights):
    device = lax.axis_index("grp") * lax.axis_size("loc") + lax.axis_index("loc")
    device = device.astype(jnp.int32).reshape(1)
    token_count, width = tokens.shape
    experts, _ = chosen.shape
    hidden_units = w_gate.shape[2]
    rows = experts * PAIR_MOST
    bf16 = jnp.bfloat16

    def exchange(block):
        block = block.reshape(experts, PAIR_MOST, width)
        block = lax.all_to_all(block, AXES, split_axis=0, concat_axis=0, tiled=True)
        return block.reshape(rows, width)

    small = pltpu.CompilerParams(vmem_limit_bytes=8 << 20)
    step = 768
    plan = [min(step, hidden_units - start) for start in range(0, hidden_units, step)]

    def hbm(array):
        return pltpu.with_memory_space_constraint(array, pltpu.HBM)

    outgoing, near = pl.pallas_call(
        dispatch_body,
        in_specs=[SMEM_SPEC, HBM_SPEC, HBM_SPEC],
        out_specs=[VMEM_SPEC] * 2,
        out_shape=[
            jax.ShapeDtypeStruct((rows, width), bf16),
            jax.ShapeDtypeStruct(chosen.shape, chosen.dtype),
        ],
        scratch_shapes=[
            pltpu.VMEM(tokens.shape, tokens.dtype),
            pltpu.SemaphoreType.DMA((2,)),
        ],
        compiler_params=small,
        name="dispatch",
    )(device, hbm(chosen), hbm(tokens))
    arrived = exchange(outgoing)
    produced, high, low = pl.pallas_call(
        lambda *refs: expert_body(token_count, plan, *refs),
        in_specs=[SMEM_SPEC] + [VMEM_SPEC] * 2 + [HBM_SPEC] * 4,
        out_specs=[VMEM_SPEC] * 3,
        out_shape=[jax.ShapeDtypeStruct((rows, width), bf16)]
        + [jax.ShapeDtypeStruct((rows, token_count), bf16)] * 2,
        scratch_shapes=[
            pltpu.VMEM(gate_weights.shape, gate_weights.dtype),
            pltpu.VMEM((width, hidden_units), bf16),
            pltpu.VMEM((width, hidden_units), bf16),
            pltpu.VMEM((hidden_units, width), bf16),
            pltpu.SemaphoreType.DMA((3, len(plan))),
            pltpu.SemaphoreType.DMA(()),
        ],
        compiler_params=pltpu.CompilerParams(vmem_limit_bytes=32 << 20),
        name="expert",
    )(device, near, arrived, hbm(gate_weights), hbm(w_gate), hbm(w_up), hbm(w_down))
    returned = exchange(produced)
    return pl.pallas_call(
        combine_body,
        in_specs=[VMEM_SPEC] * 3,
        out_specs=VMEM_SPEC,
        out_shape=jax.ShapeDtypeStruct((token_count, width), bf16),
        compiler_params=small,
        name="combine",
    )(high, low, returned)


def solution(mesh):
    return jax.shard_map(
        shards,
        mesh=mesh,
        in_specs=(
            P(AXES, None),
            P(AXES, None, None),
            P(AXES, None, None),
            P(AXES, None, None),
            P(),
            P(),
        ),
        out_specs=P(AXES, None),
        check_vma=False,
    )
```

```python
import jax
import jax.numpy as jnp
from jax import lax
from jax.experimental import pallas as pl
from jax.experimental.pallas import tpu as pltpu
from jax.sharding import PartitionSpec as P

PAIR_MOST = 8
AXES = ("grp", "loc")
VMEM_SPEC = pl.BlockSpec(memory_space=pltpu.VMEM)
SMEM_SPEC = pl.BlockSpec(memory_space=pltpu.SMEM)
HBM_SPEC = pl.BlockSpec(memory_space=pltpu.HBM)


def dot(left, right):
    return jnp.dot(left, right, preferred_element_type=jnp.float32)


def ranks_of(mine):
    slots = mine.shape[1]
    row = lax.broadcasted_iota(jnp.int32, (slots, slots), 0)
    col = lax.broadcasted_iota(jnp.int32, (slots, slots), 1)
    earlier = (row < col).astype(jnp.bfloat16)
    return dot(mine.astype(jnp.bfloat16), earlier).astype(jnp.int32)


def pick_rows(device, chosen, token_count, values):
    experts, slots = chosen.shape
    local = chosen - device * token_count
    mine = (local >= 0) & (local < token_count)
    rank = jnp.where(mine, ranks_of(mine.astype(jnp.float32)), -1)
    shape = (experts, PAIR_MOST, slots)
    pair_slot = lax.broadcasted_iota(jnp.int32, shape, 1)
    hit = jnp.broadcast_to(rank[:, None, :], shape) == pair_slot
    rows = experts * PAIR_MOST

    def total(array, empty):
        spread = jnp.broadcast_to(array[:, None, :], shape)
        return jnp.sum(jnp.where(hit, spread, empty), axis=2, keepdims=True).reshape(rows, 1)

    index = total((local + 1).astype(jnp.float32), 0.0).astype(jnp.int32) - 1
    return index, total(values, 0.0)


def dispatch_body(device_ref, chosen_hbm, tokens_hbm, weights_hbm, out_ref, chosen_ref, high_ref, low_ref,
                  tokens_ref, weights_ref, sems):
    copies = [
        pltpu.make_async_copy(chosen_hbm, chosen_ref, sems.at[0]),
        pltpu.make_async_copy(weights_hbm, weights_ref, sems.at[1]),
        pltpu.make_async_copy(tokens_hbm, tokens_ref, sems.at[2]),
    ]
    for copy in copies:
        copy.start()
    copies[0].wait()
    copies[1].wait()
    token_count = tokens_ref.shape[0]
    index, weight = pick_rows(device_ref[0], chosen_ref[...], token_count, weights_ref[...])
    token_iota = lax.broadcasted_iota(jnp.int32, (index.shape[0], token_count), 1)
    hit = index == token_iota
    table = jnp.where(hit, weight, 0.0)
    high = table.astype(jnp.bfloat16)
    high_ref[...] = high
    low_ref[...] = (table - high.astype(jnp.float32)).astype(jnp.bfloat16)
    copies[2].wait()
    out_ref[...] = dot(hit.astype(jnp.bfloat16), tokens_ref[...]).astype(jnp.bfloat16)


def expert_body(token_count, plan, device_ref, chosen_ref, arrived_ref, gate_hbm, up_hbm, down_hbm,
                out_ref, gate_ref, up_ref, down_ref, sems):
    chunks = []
    start = 0
    for number, size in enumerate(plan):
        span = pl.ds(start, size)
        start += size
        copies = (
            pltpu.make_async_copy(gate_hbm.at[0, :, span], gate_ref.at[:, span], sems.at[0, number]),
            pltpu.make_async_copy(up_hbm.at[0, :, span], up_ref.at[:, span], sems.at[1, number]),
            pltpu.make_async_copy(down_hbm.at[0, span], down_ref.at[span], sems.at[2, number]),
        )
        for copy in copies:
            copy.start()
        chunks.append((span, copies))
    rows = arrived_ref.shape[0]
    devices = rows // PAIR_MOST
    slots = chosen_ref.shape[1]
    row = chosen_ref[pl.ds(device_ref[0], 1), :]
    first = lax.broadcasted_iota(jnp.int32, (devices, slots), 0) * token_count
    spread = jnp.broadcast_to(row, (devices, slots))
    mine = (spread >= first) & (spread < first + token_count)
    rank = jnp.where(mine, ranks_of(mine.astype(jnp.float32)), -1)
    shape = (devices, PAIR_MOST, slots)
    pair_slot = lax.broadcasted_iota(jnp.int32, shape, 1)
    hit = jnp.broadcast_to(rank[:, None, :], shape) == pair_slot
    place = jnp.where(hit, 1.0, 0.0).reshape(rows, slots).astype(jnp.bfloat16)
    block = lax.dot_general(
        place, arrived_ref[...], (((0,), (0,)), ((), ())), preferred_element_type=jnp.float32
    ).astype(jnp.bfloat16)
    total = jnp.zeros((slots, out_ref.shape[1]), jnp.float32)
    for span, (gate_copy, up_copy, down_copy) in chunks:
        gate_copy.wait()
        gate_pre = dot(block, gate_ref[:, span])
        up_copy.wait()
        up_pre = dot(block, up_ref[:, span])
        hidden = (gate_pre / (1.0 + jnp.exp(-gate_pre)) * up_pre).astype(jnp.bfloat16)
        down_copy.wait()
        total = total + dot(hidden, down_ref[span, :])
    out_ref[...] = dot(place, total.astype(jnp.bfloat16)).astype(jnp.bfloat16)


def combine_body(high_ref, low_ref, back_ref, out_ref):
    dims = (((0,), (0,)), ((), ()))
    back = back_ref[...]
    total = lax.dot_general(high_ref[...], back, dims, preferred_element_type=jnp.float32)
    total = total + lax.dot_general(low_ref[...], back, dims, preferred_element_type=jnp.float32)
    out_ref[...] = total.astype(jnp.bfloat16)


def shards(tokens, w_gate, w_up, w_down, chosen, gate_weights):
    device = lax.axis_index("grp") * lax.axis_size("loc") + lax.axis_index("loc")
    device = device.astype(jnp.int32).reshape(1)
    token_count, width = tokens.shape
    experts, _ = chosen.shape
    hidden_units = w_gate.shape[2]
    rows = experts * PAIR_MOST
    bf16 = jnp.bfloat16

    def exchange(block):
        block = block.reshape(experts, PAIR_MOST, width)
        block = lax.all_to_all(block, AXES, split_axis=0, concat_axis=0, tiled=True)
        return block.reshape(rows, width)

    small = pltpu.CompilerParams(vmem_limit_bytes=8 << 20)
    step = 768
    plan = [min(step, hidden_units - start) for start in range(0, hidden_units, step)]

    def hbm(array):
        return pltpu.with_memory_space_constraint(array, pltpu.HBM)

    outgoing, near, high, low = pl.pallas_call(
        dispatch_body,
        in_specs=[SMEM_SPEC] + [HBM_SPEC] * 3,
        out_specs=[VMEM_SPEC] * 4,
        out_shape=[
            jax.ShapeDtypeStruct((rows, width), bf16),
            jax.ShapeDtypeStruct(chosen.shape, chosen.dtype),
            jax.ShapeDtypeStruct((rows, token_count), bf16),
            jax.ShapeDtypeStruct((rows, token_count), bf16),
        ],
        scratch_shapes=[
            pltpu.VMEM(tokens.shape, tokens.dtype),
            pltpu.VMEM(gate_weights.shape, gate_weights.dtype),
            pltpu.SemaphoreType.DMA((3,)),
        ],
        compiler_params=small,
        name="dispatch",
    )(device, hbm(chosen), hbm(tokens), hbm(gate_weights))
    arrived = exchange(outgoing)
    produced = pl.pallas_call(
        lambda *refs: expert_body(token_count, plan, *refs),
        in_specs=[SMEM_SPEC] + [VMEM_SPEC] * 2 + [HBM_SPEC] * 3,
        out_specs=VMEM_SPEC,
        out_shape=jax.ShapeDtypeStruct((rows, width), bf16),
        scratch_shapes=[
            pltpu.VMEM((width, hidden_units), bf16),
            pltpu.VMEM((width, hidden_units), bf16),
            pltpu.VMEM((hidden_units, width), bf16),
            pltpu.SemaphoreType.DMA((3, len(plan))),
        ],
        compiler_params=pltpu.CompilerParams(vmem_limit_bytes=32 << 20),
        name="expert",
    )(device, near, arrived, hbm(w_gate), hbm(w_up), hbm(w_down))
    returned = exchange(produced)
    return pl.pallas_call(
        combine_body,
        in_specs=[VMEM_SPEC] * 3,
        out_specs=VMEM_SPEC,
        out_shape=jax.ShapeDtypeStruct((token_count, width), bf16),
        compiler_params=small,
        name="combine",
    )(high, low, returned)


def solution(mesh):
    return jax.shard_map(
        shards,
        mesh=mesh,
        in_specs=(
            P(AXES, None),
            P(AXES, None, None),
            P(AXES, None, None),
            P(AXES, None, None),
            P(),
            P(),
        ),
        out_specs=P(AXES, None),
        check_vma=False,
    )
```

```python
import jax
import jax.numpy as jnp
from jax import lax
from jax.experimental import pallas as pl
from jax.experimental.pallas import tpu as pltpu
from jax.sharding import PartitionSpec as P

PAIR_MOST = 8
AXES = ("grp", "loc")
VMEM_SPEC = pl.BlockSpec(memory_space=pltpu.VMEM)
SMEM_SPEC = pl.BlockSpec(memory_space=pltpu.SMEM)
HBM_SPEC = pl.BlockSpec(memory_space=pltpu.HBM)


def dot(left, right):
    return jnp.dot(left, right, preferred_element_type=jnp.float32)


def ranks_of(mine):
    slots = mine.shape[1]
    row = lax.broadcasted_iota(jnp.int32, (slots, slots), 0)
    col = lax.broadcasted_iota(jnp.int32, (slots, slots), 1)
    earlier = (row < col).astype(jnp.bfloat16)
    return dot(mine.astype(jnp.bfloat16), earlier).astype(jnp.int32)


def pick_rows(device, chosen, token_count, values):
    experts, slots = chosen.shape
    local = chosen - device * token_count
    mine = (local >= 0) & (local < token_count)
    rank = jnp.where(mine, ranks_of(mine.astype(jnp.float32)), -1)
    shape = (experts, PAIR_MOST, slots)
    pair_slot = lax.broadcasted_iota(jnp.int32, shape, 1)
    hit = jnp.broadcast_to(rank[:, None, :], shape) == pair_slot
    rows = experts * PAIR_MOST

    def total(array, empty):
        spread = jnp.broadcast_to(array[:, None, :], shape)
        return jnp.sum(jnp.where(hit, spread, empty), axis=2, keepdims=True).reshape(rows, 1)

    index = total((local + 1).astype(jnp.float32), 0.0).astype(jnp.int32) - 1
    return index, total(values, 0.0)


def dispatch_body(device_ref, chosen_hbm, tokens_hbm, weights_hbm, gate_hbm, up_hbm,
                  out_ref, chosen_ref, high_ref, low_ref, gate_ref, up_ref, tokens_ref, weights_ref, sems):
    copies = [
        pltpu.make_async_copy(chosen_hbm, chosen_ref, sems.at[0]),
        pltpu.make_async_copy(weights_hbm, weights_ref, sems.at[1]),
        pltpu.make_async_copy(tokens_hbm, tokens_ref, sems.at[2]),
        pltpu.make_async_copy(gate_hbm.at[0, :, pl.ds(0, gate_ref.shape[1])], gate_ref, sems.at[3]),
        pltpu.make_async_copy(up_hbm.at[0, :, pl.ds(0, up_ref.shape[1])], up_ref, sems.at[4]),
    ]
    for copy in copies:
        copy.start()
    copies[0].wait()
    copies[1].wait()
    token_count = tokens_ref.shape[0]
    index, weight = pick_rows(device_ref[0], chosen_ref[...], token_count, weights_ref[...])
    token_iota = lax.broadcasted_iota(jnp.int32, (index.shape[0], token_count), 1)
    hit = index == token_iota
    table = jnp.where(hit, weight, 0.0)
    high = table.astype(jnp.bfloat16)
    high_ref[...] = high
    low_ref[...] = (table - high.astype(jnp.float32)).astype(jnp.bfloat16)
    copies[2].wait()
    out_ref[...] = dot(hit.astype(jnp.bfloat16), tokens_ref[...]).astype(jnp.bfloat16)
    copies[3].wait()
    copies[4].wait()


def expert_body(token_count, plan, device_ref, chosen_ref, arrived_ref, gate_first, up_first, gate_hbm, up_hbm, down_hbm,
                out_ref, gate_ref, up_ref, down_ref, sems):
    chunks = []
    start = 0
    for number, size in enumerate(plan):
        span = pl.ds(start, size)
        start += size
        copies = (
            pltpu.make_async_copy(gate_hbm.at[0, :, span], gate_ref.at[:, span], sems.at[0, number]),
            pltpu.make_async_copy(up_hbm.at[0, :, span], up_ref.at[:, span], sems.at[1, number]),
            pltpu.make_async_copy(down_hbm.at[0, span], down_ref.at[span], sems.at[2, number]),
        )
        for copy in copies if number else copies[2:]:
            copy.start()
        chunks.append((span, copies))
    rows = arrived_ref.shape[0]
    devices = rows // PAIR_MOST
    slots = chosen_ref.shape[1]
    row = chosen_ref[pl.ds(device_ref[0], 1), :]
    first = lax.broadcasted_iota(jnp.int32, (devices, slots), 0) * token_count
    spread = jnp.broadcast_to(row, (devices, slots))
    mine = (spread >= first) & (spread < first + token_count)
    rank = jnp.where(mine, ranks_of(mine.astype(jnp.float32)), -1)
    shape = (devices, PAIR_MOST, slots)
    pair_slot = lax.broadcasted_iota(jnp.int32, shape, 1)
    hit = jnp.broadcast_to(rank[:, None, :], shape) == pair_slot
    place = jnp.where(hit, 1.0, 0.0).reshape(rows, slots).astype(jnp.bfloat16)
    block = lax.dot_general(
        place, arrived_ref[...], (((0,), (0,)), ((), ())), preferred_element_type=jnp.float32
    ).astype(jnp.bfloat16)
    total = jnp.zeros((slots, out_ref.shape[1]), jnp.float32)
    for number, (span, (gate_copy, up_copy, down_copy)) in enumerate(chunks):
        if number:
            gate_copy.wait()
            gate_pre = dot(block, gate_ref[:, span])
            up_copy.wait()
            up_pre = dot(block, up_ref[:, span])
        else:
            gate_pre = dot(block, gate_first[...])
            up_pre = dot(block, up_first[...])
        hidden = (gate_pre / (1.0 + jnp.exp(-gate_pre)) * up_pre).astype(jnp.bfloat16)
        down_copy.wait()
        total = total + dot(hidden, down_ref[span, :])
    out_ref[...] = dot(place, total.astype(jnp.bfloat16)).astype(jnp.bfloat16)


def combine_body(high_ref, low_ref, back_ref, out_ref):
    dims = (((0,), (0,)), ((), ()))
    back = back_ref[...]
    total = lax.dot_general(high_ref[...], back, dims, preferred_element_type=jnp.float32)
    total = total + lax.dot_general(low_ref[...], back, dims, preferred_element_type=jnp.float32)
    out_ref[...] = total.astype(jnp.bfloat16)


def shards(tokens, w_gate, w_up, w_down, chosen, gate_weights):
    device = lax.axis_index("grp") * lax.axis_size("loc") + lax.axis_index("loc")
    device = device.astype(jnp.int32).reshape(1)
    token_count, width = tokens.shape
    experts, _ = chosen.shape
    hidden_units = w_gate.shape[2]
    rows = experts * PAIR_MOST
    bf16 = jnp.bfloat16

    def exchange(block):
        block = block.reshape(experts, PAIR_MOST, width)
        block = lax.all_to_all(block, AXES, split_axis=0, concat_axis=0, tiled=True)
        return block.reshape(rows, width)

    small = pltpu.CompilerParams(vmem_limit_bytes=8 << 20)
    step = 768
    plan = [min(step, hidden_units - start) for start in range(0, hidden_units, step)]

    def hbm(array):
        return pltpu.with_memory_space_constraint(array, pltpu.HBM)

    outgoing, near, high, low, gate_first, up_first = pl.pallas_call(
        dispatch_body,
        in_specs=[SMEM_SPEC] + [HBM_SPEC] * 5,
        out_specs=[VMEM_SPEC] * 6,
        out_shape=[
            jax.ShapeDtypeStruct((rows, width), bf16),
            jax.ShapeDtypeStruct(chosen.shape, chosen.dtype),
            jax.ShapeDtypeStruct((rows, token_count), bf16),
            jax.ShapeDtypeStruct((rows, token_count), bf16),
            pltpu.VMEM((width, plan[0]), bf16),
            pltpu.VMEM((width, plan[0]), bf16),
        ],
        scratch_shapes=[
            pltpu.VMEM(tokens.shape, tokens.dtype),
            pltpu.VMEM(gate_weights.shape, gate_weights.dtype),
            pltpu.SemaphoreType.DMA((5,)),
        ],
        compiler_params=small,
        name="dispatch",
    )(device, hbm(chosen), hbm(tokens), hbm(gate_weights), hbm(w_gate), hbm(w_up))
    arrived = exchange(outgoing)
    produced = pl.pallas_call(
        lambda *refs: expert_body(token_count, plan, *refs),
        in_specs=[SMEM_SPEC] + [VMEM_SPEC] * 4 + [HBM_SPEC] * 3,
        out_specs=VMEM_SPEC,
        out_shape=jax.ShapeDtypeStruct((rows, width), bf16),
        scratch_shapes=[
            pltpu.VMEM((width, hidden_units), bf16),
            pltpu.VMEM((width, hidden_units), bf16),
            pltpu.VMEM((hidden_units, width), bf16),
            pltpu.SemaphoreType.DMA((3, len(plan))),
        ],
        compiler_params=pltpu.CompilerParams(vmem_limit_bytes=32 << 20),
        name="expert",
    )(device, near, arrived, gate_first, up_first, hbm(w_gate), hbm(w_up), hbm(w_down))
    returned = exchange(produced)
    return pl.pallas_call(
        combine_body,
        in_specs=[VMEM_SPEC] * 3,
        out_specs=VMEM_SPEC,
        out_shape=jax.ShapeDtypeStruct((token_count, width), bf16),
        compiler_params=small,
        name="combine",
    )(high, low, returned)


def solution(mesh):
    return jax.shard_map(
        shards,
        mesh=mesh,
        in_specs=(
            P(AXES, None),
            P(AXES, None, None),
            P(AXES, None, None),
            P(AXES, None, None),
            P(),
            P(),
        ),
        out_specs=P(AXES, None),
        check_vma=False,
    )
```
